32 devices in a mesh: dp: 4 (over z), mp: 8 (over y, x, core).
Axes of the slice: x: 2, y: 2, z: 4, core: 2. Of those that a mesh axis runs over, the one named last changes fastest.
Arguments:
- inputs: bfloat16 [197, 49152], P(None, ('dp', 'mp')), may hold values from -6 to 6
- cotangent: bfloat16 [197, 49152], P(None, ('dp', 'mp')), may hold values from -1.1953125 to 1.1953125
- w_in: bfloat16 [768, 3072], P('dp', 'mp'), may hold values from -0.21875 to 0.21875
- w_out: bfloat16 [3072, 768], P('mp', 'dp'), may hold values from -0.109375 to 0.109375
- prec_in: float32 [768, 3072], P('dp', 'mp'), may hold values from 0.1 to 2
- prec_out: float32 [3072, 768], P('mp', 'dp'), may hold values from 0.1 to 2
Outputs:
- new_prec_in: float32 [768, 3072], P('dp', 'mp')
- new_prec_out: float32 [3072, 768], P('mp', 'dp')
- new_w_in: float32 [768, 3072], P('dp', 'mp')
- new_w_out: float32 [3072, 768], P('mp', 'dp')
The draws below stay inside these ranges and needn't reach their ends.
All inputs are finite; a program needn't handle non-finite values.
Results may differ from the reference program's by a relative error of at most 0.0028.
Values may be sent and summed in bfloat16 or wider, within the bound.
A program may use at most 64 MiB of HBM per device.

```python
import math
import jax
import jax.numpy as jnp
from jax import lax

D = 768
HID = 3072
SEQ = 197
IMAGES = 64


def shard_levels(own_key, extent, cuts, least, high):
    factor_of = 1.0
    for axis_at, parts in cuts:
        heights = jax.random.uniform(jax.random.fold_in(jax.random.fold_in(own_key, 6), axis_at), (parts,), jnp.float32, least / len(cuts), high / len(cuts))
        factor_of = factor_of * jnp.repeat(jnp.exp(heights), extent[axis_at] // parts).reshape((-1,) + (1,) * (len(extent) - 1 - axis_at))
    return factor_of


def centred(rng, extent, deviation, bound, shards=(), held_as=jnp.bfloat16):
    values = deviation * jax.random.normal(rng, extent, jnp.float32)
    if shards:
        values = values * shard_levels(rng, extent, shards, -0.22, 0.18)
    return jnp.clip(values, -bound, bound).astype(held_as)


def setup_inputs(seed: int = 0) -> dict:
    key_of = jax.random.split(jax.random.key(seed), 7)
    return {
        "inputs": centred(key_of[0], (SEQ, IMAGES * D), 1.0, 6.0, ((1, 32),)),
        "cotangent": centred(key_of[1], (SEQ, IMAGES * D), 0.2, 1.1953125, ((1, 32),)),
        "w_in": centred(key_of[2], (D, HID), D ** -0.5, 0.21875, ((0, 4), (1, 8))),
        "w_out": centred(key_of[3], (HID, D), HID ** -0.5, 0.109375, ((0, 8), (1, 4))),
        "prec_in": jnp.clip(jnp.exp(math.log(2.0) - 2.9957323 * jax.random.uniform(key_of[4], (D, HID), jnp.float32) ** shard_levels(key_of[4], (D, HID), ((0, 4), (1, 8)), -0.2, 0.2)), 0.1, 2.0),
        "prec_out": jnp.clip(jnp.exp(math.log(2.0) - 2.9957323 * jax.random.uniform(key_of[5], (HID, D), jnp.float32) ** shard_levels(key_of[5], (HID, D), ((0, 8), (1, 4)), -0.2, 0.2)), 0.1, 2.0),
    }


def gelu_tanh(v):
    return jax.nn.gelu(v, approximate=True)

def reference(inputs, cotangent, w_in, w_out, prec_in, prec_out):
    images = inputs.shape[1] // D
    inputs3 = jnp.transpose(inputs.reshape(SEQ, images, D), (1, 0, 2))
    cot3 = jnp.transpose(cotangent.reshape(SEQ, images, D), (1, 0, 2))

    def one_image(carry, item):
        sum_in, sq_in, sum_out, sq_out = carry
        rows, grads = item
        pre = jnp.dot(rows, w_in, preferred_element_type=jnp.float32)
        act = gelu_tanh(pre).astype(jnp.bfloat16)
        back = jnp.dot(grads, w_out.T, preferred_element_type=jnp.float32)
        delta = jax.vjp(gelu_tanh, pre)[1](back)[0].astype(jnp.bfloat16)
        g_in = jnp.dot(rows.T, delta, preferred_element_type=jnp.float32)
        g_out = jnp.dot(act.T, grads, preferred_element_type=jnp.float32)
        return ((sum_in + g_in, sq_in + g_in * g_in, sum_out + g_out, sq_out + g_out * g_out), None)
    zeros_in = jnp.zeros((D, HID), jnp.float32)
    zeros_out = jnp.zeros((HID, D), jnp.float32)
    totals, _ = lax.scan(one_image, (zeros_in, zeros_in, zeros_out, zeros_out), (inputs3, cot3))
    sum_in, sq_in, sum_out, sq_out = totals
    scale = 1.0 / images
    new_prec_in = 0.6 * prec_in + 0.4 * sq_in * scale
    new_prec_out = 0.6 * prec_out + 0.4 * sq_out * scale
    win = w_in.astype(jnp.float32)
    wout = w_out.astype(jnp.float32)
    new_w_in = win - 1.0 * (sum_in * scale + 0.1 * win) / (new_prec_in + 0.1)
    new_w_out = wout - 1.0 * (sum_out * scale + 0.1 * wout) / (new_prec_out + 0.1)
    return (new_prec_in, new_prec_out, new_w_in, new_w_out)
```

```python
import functools
import jax
import jax.numpy as jnp
from jax import lax
from jax.experimental import pallas as pl
from jax.experimental.pallas import tpu as pltpu
from jax.sharding import PartitionSpec as P


def gelu_tanh(v):
    return jax.nn.gelu(v, approximate=True)


def per_device(inputs, cotangent, w_in, w_out, prec_in, prec_out):
    SEQ = inputs.shape[0]
    D = w_in.shape[0] * lax.axis_size("dp")
    w_in_full, w_out_full = (
        lax.all_gather(w_in, "dp", axis=0, tiled=True),
        lax.all_gather(w_out, "dp", axis=1, tiled=True),
    )
    whole = lax.all_gather(inputs, "mp", axis=1, tiled=True)
    rows3 = whole.reshape(SEQ, -1, D)
    images = rows3.shape[1]
    pre = jnp.einsum("snd,dh->snh", rows3, w_in_full, preferred_element_type=jnp.float32)
    act = gelu_tanh(pre).astype(jnp.bfloat16)
    cot_whole = lax.all_gather(cotangent, "mp", axis=1, tiled=True)
    cot3 = cot_whole.reshape(SEQ, images, D)
    back = jnp.einsum("snd,hd->snh", cot3, w_out_full, preferred_element_type=jnp.float32)
    per_out = jnp.einsum("snh,snd->nhd", act, cot3, preferred_element_type=jnp.float32)
    sum_out = jnp.sum(per_out, 0)
    sq_out = jnp.sum(per_out * per_out, 0)
    delta = jax.vjp(gelu_tanh, pre)[1](back)[0].astype(jnp.bfloat16)
    rows_again = lax.all_gather(inputs, "mp", axis=1, tiled=True).reshape(SEQ, images, D)
    per_in = jnp.einsum("snd,snh->ndh", rows_again, delta, preferred_element_type=jnp.float32)
    sum_in = jnp.sum(per_in, 0)
    sq_in = jnp.sum(per_in * per_in, 0)
    sum_in, sq_in = (
        lax.psum_scatter(sum_in, "dp", scatter_dimension=0, tiled=True),
        lax.psum_scatter(sq_in, "dp", scatter_dimension=0, tiled=True),
    )
    sum_out, sq_out = (
        lax.psum_scatter(sum_out, "dp", scatter_dimension=1, tiled=True),
        lax.psum_scatter(sq_out, "dp", scatter_dimension=1, tiled=True),
    )
    scale = 1.0 / (images * lax.axis_size("dp"))
    new_prec_in = 0.6 * prec_in + 0.4 * sq_in * scale
    new_prec_out = 0.6 * prec_out + 0.4 * sq_out * scale
    w_in_own = w_in.astype(jnp.float32)
    w_out_own = w_out.astype(jnp.float32)
    new_w_in = w_in_own - 1.0 * (sum_in * scale + 0.1 * w_in_own) / (new_prec_in + 0.1)
    new_w_out = w_out_own - 1.0 * (sum_out * scale + 0.1 * w_out_own) / (new_prec_out + 0.1)
    return (new_prec_in, new_prec_out, new_w_in, new_w_out)


F32, BF16 = jnp.float32, jnp.bfloat16
NT = (((1,), (1,)), ((), ()))
MESH = pl.DeviceIdType.MESH
LANES = 128


def dot(a, b):
    return jnp.dot(a, b, preferred_element_type=F32)


def dot_nt(a, b):
    return lax.dot_general(a, b, NT, preferred_element_type=F32)


def kernel(
    x_hbm, c_hbm, win_ref, wout_t_ref, sums_in, sums_out,
    xg, cg, wg_in, wg_out, w_in_t, w_out_f, act, slope, back, delta,
    acc, own, stage, recv, passing, joined,
    loc, ici_s, ici_r, d2d_s, d2d_r, own_s, own_r, w_s, w_r, rs_s, rs_r, pass_r,
):
    z, m = lax.axis_index("dp"), lax.axis_index("mp")
    core, q = lax.rem(m, 2), m // 2
    xx, yy = lax.rem(q, 2), q // 2
    side, inner = z // 2, lax.rem((z + 1) // 2, 2)
    z_near = z + 1 - 2 * lax.rem(z, 2)

    def chip_at(s):
        return lax.rem(xx + lax.rem(s, 2), 2) + 2 * lax.rem(yy + s // 2, 2)

    chips = [chip_at(s) for s in range(4)]
    same = [2 * chip + core for chip in chips]
    other = [2 * chip + 1 - core for chip in chips]
    xn, yn, partner_id = same[1], same[2], other[0]
    depth = win_ref.shape[0]
    width = 4 * depth
    tiles = width // LANES
    x_pair = (0, 1)

    def flipped(start, size, whole, way):
        return whole - size - start + way * (2 * start + size - whole)

    def columns(start, size):
        return pl.ds(pl.multiple_of(flipped(start, size, width, side), LANES), size)

    def pair_of(k):
        return (2 + 2 * k, 3 + 2 * k)

    def view(p, mm):
        if p < 2:
            return xg.at[2 * mm + p]
        return cg.at[2 * mm + p % 2, :, columns((p - 2) // 2 * LANES, LANES)]

    def remote(src, to, ssem, rsem):
        return pltpu.make_async_remote_copy(
            src_ref=src, dst_ref=src, send_sem=ssem, recv_sem=rsem,
            device_id=(z, to), device_id_type=MESH,
        )

    def to_x(p):
        return remote(view(p, m), xn, ici_s.at[p, 0], ici_r.at[p, 0])

    def to_y(p):
        return remote(view(p, m), yn, ici_s.at[p, 1], ici_r.at[p, 1])

    def relayed(p):
        first = p % 2 == 0
        return remote(view(p, same[1 if first else 2]), yn if first else xn, ici_s.at[p, 2], ici_r.at[p, 2])

    def across(p, s):
        return remote(view(p, same[s]), partner_id, d2d_s.at[p, s - 1], d2d_r.at[p, s - 1])

    def whole_across(k, mm):
        return remote((xg, cg)[k // 2].at[2 * mm + k % 2], partner_id, own_s.at[k], own_r.at[k])

    def arrived(p, s):
        remote(view(p, same[s]), xn, ici_s.at[p, 0], ici_r.at[p, s - 1]).wait_recv()

    def from_partner(pair, s):
        for p in pair:
            remote(view(p, other[s]), partner_id, d2d_s.at[p, s - 1], d2d_r.at[p, s - 1]).wait_recv()

    def send_first(pair):
        to_x(pair[0]).start()
        to_y(pair[1]).start()

    def send_second(pair):
        to_x(pair[1]).start()
        to_y(pair[0]).start()

    def relay(pair):
        arrived(pair[0], 1)
        relayed(pair[0]).start()
        arrived(pair[1], 2)
        relayed(pair[1]).start()

    def relay_across(pair):
        across(pair[0], 1).start()
        across(pair[1], 2).start()

    def second(pair):
        arrived(pair[1], 1)
        across(pair[1], 1).start()
        arrived(pair[0], 2)
        across(pair[0], 2).start()

    def third(pair):
        for p in pair:
            arrived(p, 3)
            across(p, 3).start()

    locals_ = []
    for k in range(4):
        src, dst = ((x_hbm, xg), (c_hbm, cg))[k // 2]
        cols = pl.ds(k % 2 * width, width)
        locals_.append(pltpu.make_async_copy(src.at[:, cols], dst.at[2 * m + k % 2], loc.at[k]))
    for copy in locals_:
        copy.start()

    barrier = pltpu.get_barrier_semaphore()
    zs = [lax.rem(z + o, 4) for o in (1, 2, 3)]
    peers = [(z, xn), (z, yn), (z, partner_id)] + [(there, m) for there in zs]
    for peer in peers:
        pl.semaphore_signal(barrier, inc=1, device_id=peer, device_id_type=MESH)
    pl.semaphore_wait(barrier, len(peers))

    locals_[0].wait()
    locals_[1].wait()
    send_first(x_pair)
    send_second(x_pair)
    for k in range(2):
        whole_across(k, m).start()

    rows = pl.ds(pl.multiple_of(z * depth, 16), depth)

    def weight(k, o):
        src, dst = ((win_ref, wg_in), (wout_t_ref, wg_out))[k]
        return pltpu.make_async_remote_copy(
            src_ref=src, dst_ref=dst.at[rows], send_sem=w_s.at[k, o], recv_sem=w_r.at[k, o],
            device_id=(zs[o], m), device_id_type=MESH,
        )

    for k in range(2):
        for o in range(3):
            weight(k, o).start()
    locals_[2].wait()
    locals_[3].wait()
    send_first(pair_of(0))
    for k in range(2, 4):
        whole_across(k, m).start()
    wg_in[rows, :] = win_ref[...]
    wg_out[rows, :] = wout_t_ref[...]

    def forward(s, first, count):
        def one(j, carry):
            n = 4 * chips[s] + j
            pre = dot_nt(w_in_t[...], xg[n])
            square = pre * pre
            t = jnp.tanh(0.7978845608028654 * pre * (1.0 + 0.044715 * square))
            half = 0.5 * (1.0 + t)
            act[n] = (pre * half).astype(BF16)
            slope[n] = half + 0.5 * pre * (1.0 - t * t) * (0.7978845608028654 * (1.0 + 0.134145 * square))
            return carry
        lax.fori_loop(first, first + count, one, 0)

    def gradients(part, lhs, rhs, n, cols, fresh):
        gs = [dot(lhs[n + j], rhs[n + j, :, cols]) for j in range(4)]
        total, squares = gs[0], gs[0] * gs[0]
        for g in gs[1:]:
            total, squares = total + g, squares + g * g
        if fresh:
            acc[part, 0, :, cols] = total
            acc[part, 1, :, cols] = squares
        else:
            acc[part, 0, :, cols] += total
            acc[part, 1, :, cols] += squares

    def own_gradients(part, lhs, rhs):
        def one(k, carry):
            cols = pl.ds(pl.multiple_of(k * 2 * LANES, LANES), 2 * LANES)
            gradients(part, lhs, rhs, 4 * chips[0], cols, True)
            return carry
        lax.fori_loop(0, tiles // 2, one, 0)

    def far_gradients(part, lhs, rhs, cols):
        def one(s, carry):
            gradients(part, lhs, rhs, 4 * chip_at(s), cols, False)
            return carry
        lax.fori_loop(1, 4, one, 0)

    def backward(n, cols, fresh, last):
        for j in range(4):
            whole = dot_nt(w_out_f[:, cols], cg[n + j, :, cols])
            if not fresh:
                whole = back[n + j] + whole
            if last:
                delta[n + j] = (whole * slope[n + j]).astype(BF16)
            else:
                back[n + j] = whole

    def far_backward(k, last, sources=(1, 4)):
        cols = columns(2 * k * LANES, 2 * LANES)

        def one(s, carry):
            backward(4 * chip_at(s), cols, k == 0, last)
            return carry
        lax.fori_loop(*sources, one, 0)

    def settle(part, start, size):
        cols = columns(start, size)
        for a in range(2):
            turned = acc[part, a, :, cols].T
            own[part, a, cols, :] = turned
            stage[part, a, cols, :] = turned.astype(BF16)

    cuts = sorted({k * LANES for k in range(tiles + 1)} | {j * depth for j in range(5)})
    blocks = [(start, end - start, start // depth) for start, end in zip(cuts, cuts[1:])]

    def in_chunk(b, way):
        start, size, at = blocks[b]
        return pl.ds(pl.multiple_of(flipped(start - at * depth, size, depth, way), 16), size)

    def in_width(b):
        start, size, _ = blocks[b]
        return pl.ds(pl.multiple_of(flipped(start, size, width, side), 16), size)

    def pass_copy(part, b):
        at = blocks[b][2]
        return pltpu.make_async_remote_copy(
            src_ref=stage.at[part, :, in_width(b), :], dst_ref=passing.at[part, at, :, in_chunk(b, side), :],
            send_sem=rs_s.at[part, b], recv_sem=pass_r.at[part, b],
            device_id=(z_near, m), device_id_type=MESH,
        )

    def near_copy(part, b):
        return pltpu.make_async_remote_copy(
            src_ref=stage.at[part, :, in_width(b), :], dst_ref=recv.at[part, 0, :, in_chunk(b, side), :],
            send_sem=rs_s.at[part, b], recv_sem=rs_r.at[part, b],
            device_id=(z_near, m), device_id_type=MESH,
        )

    def joined_copy(part, b, way):
        at = blocks[b][2]
        return pltpu.make_async_remote_copy(
            src_ref=joined.at[part, at, :, in_chunk(b, side), :], dst_ref=recv.at[part, 1, :, in_chunk(b, way), :],
            send_sem=rs_s.at[part, b], recv_sem=rs_r.at[part, b],
            device_id=(3 * (1 - side) if at == 0 else 2 - side, m), device_id_type=MESH,
        )

    def inside(start, end):
        return [b for b, (first, _, _) in enumerate(blocks) if start <= first < end]

    def give(part, start, end):
        for b in inside(start, end):
            at = blocks[b][2]

            @pl.when(inner == (1 if at == 3 else 0))
            def _():
                (pass_copy if at < 2 else near_copy)(part, b).start()

    def combine(part, start, end):
        for b in inside(start, end):
            at = blocks[b][2]

            @pl.when(inner == 1)
            def _():
                pass_copy(part, b).wait_recv()
                here = in_chunk(b, side)
                for a in range(2):
                    mine = own[part, a, in_width(b), :]
                    joined[part, at, a, here, :] = (mine + passing[part, at, a, here, :].astype(F32)).astype(BF16)
                joined_copy(part, b, side).start()

    def out_step(k):
        far_gradients(0, act, cg, columns(k * LANES, LANES))
        settle(0, k * LANES, LANES)
        give(0, k * LANES, (k + 1) * LANES)

    def at_tile(k):
        return k * LANES, (k + 1) * LANES

    p0, p1, p2, p3, p4, p5 = [pair_of(k) for k in range(tiles)]

    relay(x_pair)
    send_second(p0)
    relay_across(x_pair)
    for o in range(3):
        weight(0, o).wait_recv()
    w_in_t[...] = wg_in[...].astype(F32).T.astype(BF16)
    for k in range(2):
        whole_across(k, other[0]).wait_recv()
    forward(0, 0, 4)
    for k in range(2, 4):
        whole_across(k, other[0]).wait_recv()
    own_gradients(0, act, cg)
    second(x_pair)
    relay(p0)
    send_first(p1)
    send_second(p1)
    send_first(p2)
    send_second(p2)
    relay_across(p0)
    from_partner(x_pair, 1)
    forward(1, 0, 4)
    from_partner(x_pair, 2)
    forward(2, 0, 4)
    third(x_pair)
    second(p0)
    from_partner(x_pair, 3)
    forward(3, 0, 2)
    third(p0)
    forward(3, 2, 2)
    relay(p1)
    send_first(p3)
    send_second(p3)
    relay_across(p1)
    for s in range(1, 4):
        from_partner(p0, s)
    out_step(0)
    second(p1)

    for o in range(3):
        weight(1, o).wait_recv()
    w_out_f[...] = wg_out[...].astype(F32).T.astype(BF16)
    backward(4 * chips[0], pl.ds(0, width), True, True)
    relay(p2)
    send_first(p4)
    send_second(p4)
    relay_across(p2)
    second(p2)
    third(p1)
    for s in range(1, 4):
        from_partner(p1, s)
    out_step(1)
    relay(p3)
    send_first(p5)
    send_second(p5)
    relay_across(p3)
    far_backward(0, False)
    second(p3)
    third(p2)
    combine(0, *at_tile(0))
    for s in range(1, 4):
        from_partner(p2, s)
    out_step(2)
    relay(p4)
    relay_across(p4)
    second(p4)
    own_gradients(1, delta, xg)
    third(p3)
    combine(0, *at_tile(1))
    relay(p5)
    relay_across(p5)
    for s in range(1, 4):
        from_partner(p3, s)
    out_step(3)
    far_backward(1, False)
    second(p5)
    third(p4)
    combine(0, *at_tile(2))
    third(p5)
    for s in range(1, 4):
        from_partner(p4, s)
    out_step(4)
    for s in range(1, 3):
        from_partner(p5, s)
    far_backward(2, True, (1, 3))
    from_partner(p5, 3)
    far_backward(2, True, (3, 4))

    for k in range(tiles // 2):
        start, size = 2 * k * LANES, 2 * LANES
        far_gradients(1, delta, xg, columns(start, size))
        settle(1, start, size)
        give(1, start, start + size)
        if k == 0:
            out_step(5)

    def collected(part, sums):
        for near, joint, kind in (((6, 7), (0, 1), 0), ((4, 5), (2, 3), 1)):
            @pl.when(inner == kind)
            def _():
                for b in near:
                    near_copy(part, b).wait_recv()
                for b in joint:
                    joined_copy(part, b, 1 - side).wait_recv()
        for a in range(2):
            total = own[part, a, rows, :]
            for t in range(2):
                total = total + recv[part, t, a].astype(F32)
            sums[a] = total

    collected(0, sums_out)
    combine(1, 0, 2 * depth)
    collected(1, sums_in)

    for pair in (x_pair, p0, p1, p2, p3, p4, p5):
        for p in pair:
            to_x(p).wait_send()
            to_y(p).wait_send()
            relayed(p).wait_send()
            for s in range(1, 4):
                across(p, s).wait_send()
    for k in range(4):
        whole_across(k, m).wait_send()
    for k in range(2):
        for o in range(3):
            weight(k, o).wait_send()
    for part in range(2):
        for b in range(len(blocks)):
            at = blocks[b][2]
            if at < 2:
                pass_copy(part, b).wait_send()
            else:
                @pl.when(inner == (1 if at == 3 else 0))
                def _():
                    near_copy(part, b).wait_send()


def fused(inputs, cotangent, w_in, w_out, prec_in, prec_out):
    seq, local = inputs.shape
    depth, hid = w_in.shape
    width = 4 * depth
    images = 8 * local // width
    pieces = 2 + 2 * width // LANES
    vmem, hbm = pl.BlockSpec(memory_space=pltpu.VMEM), pl.BlockSpec(memory_space=pl.ANY)
    dma = pltpu.SemaphoreType.DMA
    sums_in, sums_out = pl.pallas_call(
        kernel,
        out_shape=[jax.ShapeDtypeStruct((2, depth, hid), F32)] * 2,
        in_specs=[hbm, hbm] + [vmem] * 2,
        out_specs=[vmem] * 2,
        scratch_shapes=[
            pltpu.VMEM((images, seq, width), BF16),
            pltpu.VMEM((images, seq, width), BF16),
            pltpu.VMEM((width, hid), BF16),
            pltpu.VMEM((width, hid), BF16),
            pltpu.VMEM((hid, width), BF16),
            pltpu.VMEM((hid, width), BF16),
            pltpu.VMEM((images, hid, seq), BF16),
            pltpu.VMEM((images, hid, seq), F32),
            pltpu.VMEM((images, hid, seq), F32),
            pltpu.VMEM((images, hid, seq), BF16),
            pltpu.VMEM((2, 2, hid, width), F32),
            pltpu.VMEM((2, 2, width, hid), F32),
            pltpu.VMEM((2, 2, width, hid), BF16),
            pltpu.VMEM((2, 2, 2, depth, hid), BF16),
            pltpu.VMEM((2, 2, 2, depth, hid), BF16),
            pltpu.VMEM((2, 2, 2, depth, hid), BF16),
            dma((4,)), dma((pieces, 3)), dma((pieces, 3)), dma((pieces, 3)), dma((pieces, 3)),
            dma((4,)), dma((4,)), dma((2, 3)), dma((2, 3)), dma((2, 8)), dma((2, 8)), dma((2, 4)),
        ],
        compiler_params=pltpu.CompilerParams(
            collective_id=0, has_side_effects=True, vmem_limit_bytes=60 * 1024 * 1024
        ),
    )(inputs, cotangent, w_in, w_out.T)

    scale = 1.0 / (images * 4)

    def updated(sums, prec, w):
        new_prec = 0.6 * prec + 0.4 * sums[1] * scale
        mean = w.astype(F32)
        return new_prec, mean - 1.0 * (sums[0] * scale + 0.1 * mean) / (new_prec + 0.1)

    new_prec_in, new_w_in = updated(sums_in, prec_in, w_in)
    new_prec_out, new_w_out = updated(sums_out, prec_out.T, w_out.T)
    return new_prec_in, new_prec_out.T, new_w_in, new_w_out.T


def solution(mesh):
    placed = (
        P(None, ("dp", "mp")),
        P(None, ("dp", "mp")),
        P("dp", "mp"),
        P("mp", "dp"),
        P("dp", "mp"),
        P("mp", "dp"),
    )
    body = fused if dict(mesh.shape) == {"dp": 4, "mp": 8} else per_device
    return jax.shard_map(
        body,
        mesh=mesh,
        in_specs=placed,
        out_specs=(P("dp", "mp"), P("mp", "dp"), P("dp", "mp"), P("mp", "dp")),
        check_vma=False,
    )
```
